128 devices in a mesh: grp: 4 (over x), orient: 32 (over y, z, core).
Axes of the slice: x: 4, y: 4, z: 4, core: 2. Of those that a mesh axis runs over, the one named last changes fastest.
Arguments:
- images: bfloat16 [4096, 2, 8192], P(('grp', 'orient')), may hold values from -6 to 6
- ctf: bfloat16 [4096, 8192], P(('grp', 'orient')), may hold values from -1 to 1
- shifts: int32 [4096, 2], P(('grp', 'orient')), may hold values from -8 to 8
- home: int32 [4, 4096, 1], P(None, ('grp', 'orient')), may hold values from 0 to 31; in each aligned block of 32 rows (0 to 31, 32 to 63, ..., all dimensions but the last counted through in order) at most 2 rows name the same one
- neighbours: int32 [4096, 4, 128], P(('grp', 'orient')), may hold values from 0 to 511
- references: bfloat16 [4, 16384, 2, 8192], P('grp', 'orient'), may hold values from -6 to 6
- noise_weight: float32 [4, 8192], P('grp'), may hold values from 0.25 to 4
Outputs:
- centred: float32 [4096, 4, 128], P(('grp', 'orient'))
The draws below stay inside these ranges and needn't reach their ends.
Inputs may be any that keep to these rules, and one draw needn't show every extreme that they name: `home`: within one group, at most 2 of the 32 particles of one device share a block, and in every draw some device has exactly 2 particles in one block.
All inputs are finite; a program needn't handle non-finite values.
Results may differ from the reference program's by a relative error of at most 0.0042.
Values may be sent and summed in bfloat16 or wider, within the bound.
No kernel may reach another device: no remote copies, remote signals or barrier semaphores. Data moves between devices by JAX's collectives and lax.ppermute only.
A program may use at most 256 MiB of HBM per device.

```python
import math
import jax
import jax.numpy as jnp
import numpy as np
from jax import lax

BOX = 128
PIX = 8192
ORI_DEV = 512
NBR = 128
PART_DEV = 32
GROUPS = 4
OWNERS = 32
CAP = 2
ORIENTS = 16384
PARTS_SIZE = 4096


def touch_ends(array, key, smallest, high):
    longest = array.shape.index(max(array.shape))
    spots = []
    for shift in (0, 1):
        where = [jax.random.randint(jax.random.fold_in(key, axis), (), 0, length) for axis, length in enumerate(array.shape)]
        where[longest] = (where[longest] + shift) % array.shape[longest]
        spots.append(tuple(where))
    return array.at[spots[0]].set(smallest).at[spots[1]].set(high)


def steps_of(stream_key, shape, cuts, smallest, top_value):
    def one(axis_at, parts):
        heights = jax.random.uniform(jax.random.fold_in(jax.random.fold_in(stream_key, 6), axis_at), (parts,), jnp.float32, smallest / len(cuts), top_value / len(cuts))
        return jnp.repeat(jnp.exp(heights), shape[axis_at] // parts).reshape((-1,) + (1,) * (len(shape) - axis_at - 1))

    level = one(*cuts[0])
    for cut in cuts[1:]:
        level = level * one(*cut)
    return level


def assign_block(rng, own, number, rows, number_of, top, reach, skew):
    ranking = jax.random.permutation(rng, number_of)
    crowded, common = shares(number_of, rows * top, reach, skew, True), shares(number_of, rows * top, reach, skew, False)
    places = jnp.arange(number_of)

    def named(sizes, offset_by):
        used = int((sizes > 0).sum())
        fixed = max(1, used // 4)
        moved = fixed + (places - fixed + offset_by * (used - fixed)) % max(1, number_of - fixed)
        return jnp.zeros((number_of,), jnp.int32).at[ranking[jnp.where(places < fixed, places, moved)]].set(jnp.asarray(sizes, jnp.int32))

    sizes = jnp.where(number % 4 == 0, named(crowded, number // 4), named(common, number - number // 4 - 1))
    mixed = jax.random.permutation(jax.random.fold_in(own, 3), number_of)
    source_of, sink = mixed[0:number_of // 2 * 2:2], mixed[1:number_of // 2 * 2:2]
    room = jnp.minimum(sizes[source_of] - 1, reach - sizes[sink]) // 2
    room = jnp.where((source_of == ranking[0]) | (sink == ranking[0]) | (sizes[sink] == 0), 0, jnp.maximum(room, 0))
    moved = jax.random.randint(jax.random.fold_in(own, 4), (number_of // 2,), 0, 1 << 20) % (room + 1)
    sizes = sizes.at[source_of].add(-moved).at[sink].add(moved)
    members = jnp.searchsorted(jnp.cumsum(sizes), jnp.arange(rows * top), side="right").astype(jnp.int32)
    table = members.reshape(top, rows).T
    table = table[jax.random.permutation(jax.random.fold_in(own, 1), rows)]
    offset_by = jax.random.randint(jax.random.fold_in(own, 2), (rows, 1), 0, top)
    return jnp.take_along_axis(table, (jnp.arange(top)[None, :] + offset_by) % top, axis=1)


def shares(number_of, total, limit, slope, full):
    weights = [(1 << 20) // math.isqrt(rank ** slope) + 1 for rank in range(1, number_of + 1)]
    largest = limit if full else min(limit, max(-(-total // number_of), total * weights[0] // sum(weights)))
    least = 1 if total - largest >= number_of - 1 else 0
    counts, spare = [largest] + [least] * (number_of - 1), total - largest - least * (number_of - 1)
    while spare > 0:
        candidates = [i for i in range(1, number_of) if counts[i] < largest] or [i for i in range(1, number_of) if counts[i] < limit]
        pool, budget = sum([weights[i] for i in candidates]), spare
        for i in candidates:
            more = min(limit - counts[i], max(1, budget * weights[i] // pool), spare)
            counts[i] = counts[i] + more
            spare = spare - more
    return np.array(counts)


def gaussian(key, extent, width, bound, pieces=(), held_as=jnp.bfloat16):
    gain = steps_of(key, extent, pieces, -0.22, 0.18) if pieces else 1.0
    entries = jax.random.normal(key, extent, jnp.float32) * width * gain
    return jnp.minimum(jnp.maximum(entries, -bound), bound).astype(held_as)


def setup_inputs(seed: int = 0) -> dict:
    splits = jax.random.split(jax.random.key(seed), 8)
    images = gaussian(splits[0], (PARTS_SIZE, 2, PIX), 1.0, 6.0, ((0, 128),))
    ctf = jnp.clip(jax.random.uniform(splits[1], (PARTS_SIZE, PIX), jnp.float32, -1.0, 1.0) * steps_of(splits[1], (PARTS_SIZE, PIX), ((0, 128),), -0.4, 0.0), -1.0, 1.0).astype(jnp.bfloat16)
    shifts = touch_ends(jax.random.randint(splits[2], (PARTS_SIZE, 2), -8, 9), jax.random.fold_in(splits[2], 1), -8, 8).astype(jnp.int32)
    home_keys = jax.random.split(jax.random.fold_in(splits[3], 1), GROUPS * PARTS_SIZE // PART_DEV)
    home_turns = jax.random.permutation(jax.random.fold_in(splits[3], 3), GROUPS * PARTS_SIZE // PART_DEV)
    home = jax.vmap(lambda own, number: assign_block(jax.random.fold_in(splits[3], 2), own, number, PART_DEV, OWNERS, 1, CAP, 2))(home_keys, home_turns).reshape((GROUPS, PARTS_SIZE, 1))
    neighbours = touch_ends(jax.random.randint(splits[4], (PARTS_SIZE, GROUPS, NBR), 0, ORI_DEV), jax.random.fold_in(splits[4], 1), 0, ORI_DEV - 1).astype(jnp.int32)
    references = gaussian(splits[5], (GROUPS, ORIENTS, 2, PIX), 1.0, 6.0, ((0, 4), (1, 32)))
    noise_weight = jnp.clip(jnp.exp(math.log(4.0) - 2.7725887 * jax.random.uniform(splits[6], (GROUPS, PIX), jnp.float32) ** steps_of(splits[6], (GROUPS, PIX), ((0, 4),), -0.2, 0.2)), 0.25, 4.0)
    return dict(images=images, ctf=ctf, shifts=shifts, home=home, neighbours=neighbours, references=references, noise_weight=noise_weight)


def shift_tables(shifts, box):
    half = box // 2
    row = jnp.arange(box, dtype=jnp.int32)
    freq_y = jnp.where(row < half, row, row - box).astype(jnp.float32)
    freq_x = jnp.arange(half, dtype=jnp.int32).astype(jnp.float32)
    grid_y = jnp.broadcast_to(freq_y[:, None], (box, half)).reshape(-1)
    grid_x = jnp.broadcast_to(freq_x[None, :], (box, half)).reshape(-1)
    move_x = shifts[:, 0].astype(jnp.float32)
    move_y = shifts[:, 1].astype(jnp.float32)
    angle = -2.0 * math.pi / box * (move_x[:, None] * grid_x[None, :] + move_y[:, None] * grid_y[None, :])
    return (jnp.cos(angle), jnp.sin(angle))

def reference(images, ctf, shifts, home, neighbours, references, noise_weight):
    cosine, sine = shift_tables(shifts, BOX)
    real = images[:, 0].astype(jnp.float32)
    imag = images[:, 1].astype(jnp.float32)
    shifted = jnp.stack([real * cosine - imag * sine, real * sine + imag * cosine], axis=1).astype(jnp.bfloat16)
    ref_real = references[:, :, 0].astype(jnp.float32)
    ref_imag = references[:, :, 1].astype(jnp.float32)
    ref_power = (ref_real * ref_real + ref_imag * ref_imag).astype(jnp.bfloat16)
    orientation = jnp.transpose(home[:, :, 0]).astype(jnp.int32)[:, :, None] * ORI_DEV + neighbours.astype(jnp.int32)
    scale = 1.0 / math.sqrt(PIX)

    def score_one(item):
        shifted_p, ctf_p, picks_all = item
        ctf_f = ctf_p.astype(jnp.float32)

        def per_group(weight, blocks, powers, picks):
            tone = weight * ctf_f
            weighted = (tone[None, :] * shifted_p.astype(jnp.float32)).astype(jnp.bfloat16).reshape(-1)
            tone_power = (tone * ctf_f).astype(jnp.bfloat16)
            chosen = blocks[picks].reshape(picks.shape[0], -1)
            cross = jnp.dot(chosen, weighted, preferred_element_type=jnp.float32)
            power = jnp.dot(powers[picks], tone_power, preferred_element_type=jnp.float32)
            return (power - 2.0 * cross) * scale
        return jax.vmap(per_group)(noise_weight, references, ref_power, picks_all)
    score = lax.map(score_one, (shifted, ctf, orientation))
    return score - lax.optimization_barrier(jnp.mean(score, axis=2, keepdims=True))
```

```python
import math

import jax
import jax.numpy as jnp
from jax import lax
from jax.experimental import pallas as pl
from jax.experimental.pallas import tpu as pltpu
from jax.sharding import PartitionSpec as P

BOX = 128
PIX = 8192
LANES = 128
SLABS = PIX // LANES
CHUNKS = 2
GROUP = 8


def rotation(move_x, move_y, slab):
    lane = lax.broadcasted_iota(jnp.int32, move_x.shape, 1)
    row = 2 * slab + jnp.where(lane >= 64, 1, 0) - jnp.where(slab >= SLABS // 2, BOX, 0)
    turns = move_x * (lane & 63).astype(jnp.float32) + move_y * row.astype(jnp.float32)
    quarter = jnp.round(turns * (1.0 / 32.0))
    phi = (turns - 32.0 * quarter) * (2.0 * math.pi / BOX)
    sq = phi * phi
    sine = phi * (1.0 + sq * (-1.0 / 6 + sq * (1.0 / 120 + sq * (-1.0 / 5040 + sq * (1.0 / 362880)))))
    cosine = 1.0 + sq * (-0.5 + sq * (1.0 / 24 + sq * (-1.0 / 720 + sq * (1.0 / 40320))))
    step = quarter.astype(jnp.int32) & 3
    swap = (step & 1) == 1
    base_c = jnp.where(swap, sine, cosine)
    base_s = jnp.where(swap, cosine, sine)
    return (
        jnp.where((step == 1) | (step == 2), -base_c, base_c),
        jnp.where(step >= 2, -base_s, base_s),
    )


def pack_kernel(chunk, width, shift_ref, select_ref, real_ref, imag_ref, ctf_ref, out_ref):
    local = shift_ref.shape[0]
    devices, _, slots, _ = out_ref.shape
    move_x = jnp.broadcast_to(shift_ref[:, 0:1].astype(jnp.float32), (local, LANES))
    move_y = jnp.broadcast_to(shift_ref[:, 1:2].astype(jnp.float32), (local, LANES))

    def one(r, carry):
        cols = pl.ds(pl.multiple_of(r * LANES, LANES), LANES)
        cosine, sine = rotation(move_x, move_y, chunk * width + r)
        real = real_ref[:, cols].astype(jnp.float32)
        imag = imag_ref[:, cols].astype(jnp.float32)
        payload = jnp.concatenate(
            [
                (real * cosine + imag * sine).astype(jnp.bfloat16),
                (imag * cosine - real * sine).astype(jnp.bfloat16),
                ctf_ref[:, cols],
            ],
            axis=1,
        )
        packed = jnp.dot(
            select_ref[...], payload, preferred_element_type=jnp.float32
        ).astype(jnp.bfloat16)
        for part in range(3):
            piece = packed[:, part * LANES : (part + 1) * LANES]
            out_ref[:, part * width + r] = piece.reshape(devices, slots, LANES)
        return carry

    lax.fori_loop(0, width, one, 0, unroll=2)


def pack(chunk, shifts, select, real, imag, ctf, devices, slots):
    local = shifts.shape[0]
    width = SLABS // CHUNKS
    block = pl.BlockSpec((local, width * LANES), lambda i: (0, chunk))
    whole = lambda array: pl.BlockSpec(array.shape, lambda i: (0, 0))
    shape = (devices, 3 * width, slots, LANES)

    def body(*refs):
        pack_kernel(chunk, width, *refs)

    return pl.pallas_call(
        body,
        grid=(1,),
        in_specs=[whole(shifts), whole(select), block, block, block],
        out_specs=pl.BlockSpec(shape, lambda i: (0, 0, 0, 0)),
        out_shape=jax.ShapeDtypeStruct(shape, jnp.bfloat16),
        cost_estimate=pl.CostEstimate(
            flops=2 * devices * slots * local * 3 * width * LANES,
            bytes_accessed=2 * 3 * width * LANES * (devices * slots + local),
            transcendentals=0,
        ),
        compiler_params=pltpu.CompilerParams(vmem_limit_bytes=48 * 2**20),
        name=f"pack_{chunk}",
    )(shifts, select, real, imag, ctf)


def match_kernel(arrived_ref, base_ref, weight_ref, re_ref, im_ref, pw_ref, out_ref):
    @pl.when(pl.program_id(0) == 0)
    def _():
        out_ref[...] = base_ref[...]

    rows = out_ref.shape[0]
    sides = ([], [], [])
    for r in range(GROUP):
        real, imag, ctf = (
            arrived_ref[:, part, r].reshape(rows, LANES).astype(jnp.float32) for part in range(3)
        )
        tone = ctf * weight_ref[:, r * LANES : (r + 1) * LANES]
        for side, value in zip(sides, (real, imag, ctf)):
            side.append((tone * value).astype(jnp.bfloat16))
    contract = (((1,), (1,)), ((), ()))
    scale = 1.0 / math.sqrt(PIX)
    cross = lax.dot_general(
        jnp.concatenate(sides[0], axis=1), re_ref[...], contract, preferred_element_type=jnp.float32
    ) + lax.dot_general(
        jnp.concatenate(sides[1], axis=1), im_ref[...], contract, preferred_element_type=jnp.float32
    )
    power = lax.dot_general(
        jnp.concatenate(sides[2], axis=1), pw_ref[...], contract, preferred_element_type=jnp.float32
    )
    out_ref[...] += (power - 2.0 * cross) * scale


def match(chunk, arrived, base, weight, tables):
    devices, depth, slots, _ = arrived.shape
    width = depth // 3
    steps = width // GROUP
    orients = tables[0].shape[0]
    arrived = arrived.reshape(devices, 3, width, slots, LANES)
    table = pl.BlockSpec((orients, GROUP * LANES), lambda i: (0, chunk * steps + i))
    full = pl.BlockSpec((devices * slots, orients), lambda i: (0, 0))
    return pl.pallas_call(
        match_kernel,
        grid=(steps,),
        in_specs=[
            pl.BlockSpec((devices, 3, GROUP, slots, LANES), lambda i: (0, 0, i, 0, 0)),
            full,
            pl.BlockSpec((1, GROUP * LANES), lambda i: (0, chunk * steps + i)),
            table,
            table,
            table,
        ],
        out_specs=full,
        out_shape=jax.ShapeDtypeStruct((devices * slots, orients), jnp.float32),
        cost_estimate=pl.CostEstimate(
            flops=2 * devices * slots * orients * depth * LANES,
            bytes_accessed=2 * depth * LANES * (devices * slots + orients),
            transcendentals=0,
        ),
        compiler_params=pltpu.CompilerParams(vmem_limit_bytes=48 * 2**20),
        name=f"match_{chunk}",
    )(arrived, base, weight, *tables)


def pick_kernel(rows_ref, near_ref, out_ref):
    near = near_ref[...]
    lane = near & (LANES - 1)
    band = near // LANES
    picked = jnp.zeros(near.shape, jnp.float32)
    for at in range(rows_ref.shape[1] // LANES):
        piece = rows_ref[:, at * LANES : (at + 1) * LANES]
        found = jnp.take_along_axis(piece, lane, axis=1)
        picked = jnp.where(band == at, found, picked)
    out_ref[...] = picked - jnp.mean(picked, axis=1, keepdims=True)


def pick(rows, near):
    return pl.pallas_call(
        pick_kernel,
        out_shape=jax.ShapeDtypeStruct(near.shape, jnp.float32),
        name="pick",
    )(rows, near)


def per_device(images, ctf, shifts, home, neighbours, references, noise_weight):
    groups = home.shape[0]
    owners = lax.axis_size("orient")
    devices = groups * owners
    local = images.shape[0]
    slots = max(2, 2 * local // owners)
    total = devices * slots
    target = home[:, :, 0]
    earlier = jnp.arange(local)[:, None] > jnp.arange(local)[None, :]
    same = target[:, :, None] == target[:, None, :]
    rank = jnp.sum((same & earlier[None]).astype(jnp.int32), axis=2)
    slot = (jnp.arange(groups, dtype=jnp.int32)[:, None] * owners + target) * slots + rank
    select = jnp.sum(
        (slot[:, None, :] == jnp.arange(total, dtype=jnp.int32)[None, :, None]).astype(jnp.int32),
        axis=0,
    ).astype(jnp.bfloat16)
    real, imag = images[:, 0], images[:, 1]
    sent = [pack(c, shifts, select, real, imag, ctf, devices, slots) for c in range(CHUNKS)]
    arrived = [
        lax.all_to_all(s, ("grp", "orient"), split_axis=0, concat_axis=0, tiled=True) for s in sent
    ]
    ref_real, ref_imag = references[0, :, 0], references[0, :, 1]
    wide_real, wide_imag = ref_real.astype(jnp.float32), ref_imag.astype(jnp.float32)
    ref_power = (wide_real * wide_real + wide_imag * wide_imag).astype(jnp.bfloat16)
    tables = (ref_real, ref_imag, ref_power)
    score = jnp.zeros((total, references.shape[1]), jnp.float32)
    for c in range(CHUNKS):
        score = match(c, arrived[c], score, noise_weight, tables)
    returned = lax.all_to_all(
        score.reshape(devices, slots, -1), ("grp", "orient"), split_axis=0, concat_axis=0, tiled=True
    )
    flat_back = returned.reshape(total, -1)
    chosen = (
        slot.T.reshape(-1)[:, None] == jnp.arange(total, dtype=jnp.int32)[None, :]
    ).astype(jnp.float32)
    mine = jnp.dot(chosen, flat_back, precision=lax.Precision.HIGHEST)
    return pick(mine, neighbours.reshape(local * groups, -1)).reshape(local, groups, -1)


def solution(mesh):
    in_specs = (
        P(("grp", "orient"), None, None),
        P(("grp", "orient"), None),
        P(("grp", "orient"), None),
        P(None, ("grp", "orient"), None),
        P(("grp", "orient"), None, None),
        P("grp", "orient", None, None),
        P("grp", None),
    )
    out_specs = P(("grp", "orient"), None, None)
    return jax.shard_map(
        per_device, mesh=mesh, in_specs=in_specs, out_specs=out_specs, check_vma=False
    )
```

```python
import math

import jax
import jax.numpy as jnp
from jax import lax
from jax.experimental import pallas as pl
from jax.experimental.pallas import tpu as pltpu
from jax.sharding import PartitionSpec as P

BOX = 128
PIX = 8192
LANES = 128
SLABS = PIX // LANES
CHUNKS = 2
GROUP = 8
NEAR = 128


def rotation(move_x, move_y, slab):
    lane = lax.broadcasted_iota(jnp.int32, move_x.shape, 1)
    row = 2 * slab + jnp.where(lane >= 64, 1, 0) - jnp.where(slab >= SLABS // 2, BOX, 0)
    turns = move_x * (lane & 63).astype(jnp.float32) + move_y * row.astype(jnp.float32)
    quarter = jnp.round(turns * (1.0 / 32.0))
    phi = (turns - 32.0 * quarter) * (2.0 * math.pi / BOX)
    sq = phi * phi
    sine = phi * (1.0 + sq * (-1.0 / 6 + sq * (1.0 / 120 + sq * (-1.0 / 5040 + sq * (1.0 / 362880)))))
    cosine = 1.0 + sq * (-0.5 + sq * (1.0 / 24 + sq * (-1.0 / 720 + sq * (1.0 / 40320))))
    step = quarter.astype(jnp.int32) & 3
    swap = (step & 1) == 1
    base_c = jnp.where(swap, sine, cosine)
    base_s = jnp.where(swap, cosine, sine)
    return (
        jnp.where((step == 1) | (step == 2), -base_c, base_c),
        jnp.where(step >= 2, -base_s, base_s),
    )


def pack_kernel(chunk, width, shift_ref, slot_ref, image_ref, ctf_ref, near_ref, out_ref, pair_ref):
    local = shift_ref.shape[0]
    groups = slot_ref.shape[0]
    devices, depth, slots, _ = out_ref.shape
    total = devices * slots
    move_x = jnp.broadcast_to(shift_ref[:, 0:1].astype(jnp.float32), (local, LANES))
    move_y = jnp.broadcast_to(shift_ref[:, 1:2].astype(jnp.float32), (local, LANES))
    place = lax.broadcasted_iota(jnp.int32, (total, local), 0)
    hit = place == slot_ref[0:1, :]
    for g in range(1, groups):
        hit = hit | (place == slot_ref[g : g + 1, :])
    select = jnp.where(hit, 1.0, 0.0).astype(jnp.bfloat16)

    def spread(rows, payload):
        return jnp.dot(rows, payload, preferred_element_type=jnp.float32).astype(jnp.bfloat16)

    def one(r, carry):
        cols = pl.ds(pl.multiple_of(r * LANES, LANES), LANES)
        cosine, sine = rotation(move_x, move_y, chunk * width + r)
        pair_ref[...] = image_ref[:, :, cols].reshape(2 * local, LANES).astype(jnp.float32)
        real = pair_ref[pl.ds(0, local, stride=2), :]
        imag = pair_ref[pl.ds(1, local, stride=2), :]
        payload = jnp.concatenate(
            [
                (real * cosine + imag * sine).astype(jnp.bfloat16),
                (imag * cosine - real * sine).astype(jnp.bfloat16),
                ctf_ref[:, cols],
            ],
            axis=1,
        )
        packed = spread(select, payload)
        for part in range(3):
            piece = packed[:, part * LANES : (part + 1) * LANES]
            out_ref[:, 3 * r + part] = piece.reshape(devices, slots, LANES)
        return carry

    lax.fori_loop(0, width, one, 0, unroll=2)
    if depth > 3 * width:
        share = total // groups
        halves = ([], [])
        for g in range(groups):
            near = near_ref[:, g * NEAR : (g + 1) * NEAR]
            for half, value in zip(halves, (near >> 1, near & 1)):
                half.append(
                    spread(select[g * share : (g + 1) * share], value.astype(jnp.float32).astype(jnp.bfloat16))
                )
        for at, half in enumerate(halves):
            out_ref[:, 3 * width + at] = jnp.concatenate(half, axis=0).reshape(devices, slots, NEAR)


def pack(chunk, shifts, slot, images, ctf, near, devices, slots):
    local = shifts.shape[0]
    width = SLABS // CHUNKS
    span = width * LANES
    depth = 3 * width + (2 if chunk == CHUNKS - 1 else 0)
    whole = lambda array: pl.BlockSpec(array.shape, lambda i: (0, 0))
    shape = (devices, depth, slots, LANES)

    def body(*refs):
        pack_kernel(chunk, width, *refs)

    return pl.pallas_call(
        body,
        grid=(1,),
        in_specs=[
            whole(shifts),
            whole(slot),
            pl.BlockSpec((local, 2, span), lambda i: (0, 0, chunk)),
            pl.BlockSpec((local, span), lambda i: (0, chunk)),
            whole(near),
        ],
        out_specs=pl.BlockSpec(shape, lambda i: (0, 0, 0, 0)),
        out_shape=jax.ShapeDtypeStruct(shape, jnp.bfloat16),
        scratch_shapes=[pltpu.VMEM((2 * local, LANES), jnp.float32)],
        cost_estimate=pl.CostEstimate(
            flops=2 * devices * slots * local * depth * LANES,
            bytes_accessed=2 * depth * LANES * (devices * slots + local),
            transcendentals=0,
        ),
        compiler_params=pltpu.CompilerParams(vmem_limit_bytes=48 * 2**20),
        name=f"pack_{chunk}",
    )(shifts, slot, images, ctf, near)


def table_kernel(block_ref, after_ref, re_ref, im_ref, pw_ref, pair_ref):
    rows, _, span = block_ref.shape

    def one(r, carry):
        cols = pl.ds(pl.multiple_of(r * LANES, LANES), LANES)
        pair_ref[...] = block_ref[:, :, cols].reshape(2 * rows, LANES).astype(jnp.float32)
        real = pair_ref[pl.ds(0, rows, stride=2), :]
        imag = pair_ref[pl.ds(1, rows, stride=2), :]
        re_ref[:, cols] = real.astype(jnp.bfloat16)
        im_ref[:, cols] = imag.astype(jnp.bfloat16)
        pw_ref[:, cols] = (real * real + imag * imag).astype(jnp.bfloat16)
        return carry

    lax.fori_loop(0, span // LANES, one, 0, unroll=4)


def tabulate(blocks, after):
    orients = blocks.shape[0]
    rows = 64
    out = pl.BlockSpec((rows, PIX), lambda i: (i, 0))
    return pl.pallas_call(
        table_kernel,
        grid=(orients // rows,),
        in_specs=[
            pl.BlockSpec((rows, 2, PIX), lambda i: (i, 0, 0)),
            pl.BlockSpec(memory_space=pl.ANY),
        ],
        out_specs=[out] * 3,
        out_shape=[jax.ShapeDtypeStruct((orients, PIX), jnp.bfloat16)] * 3,
        scratch_shapes=[pltpu.VMEM((2 * rows, LANES), jnp.float32)],
        cost_estimate=pl.CostEstimate(
            flops=2 * orients * PIX * 1024, bytes_accessed=10 * orients * PIX, transcendentals=0
        ),
        name="tabulate",
    )(blocks, after)


def accumulate(arrived_ref, weight_ref, re_ref, im_ref, pw_ref, total_ref):
    rows = total_ref.shape[0]
    sides = ([], [], [])
    for r in range(GROUP):
        real, imag, ctf = (
            arrived_ref[:, 3 * r + part].reshape(rows, LANES).astype(jnp.float32)
            for part in range(3)
        )
        tone = ctf * weight_ref[:, r * LANES : (r + 1) * LANES]
        for side, value in zip(sides, (real, imag, ctf)):
            side.append((tone * value).astype(jnp.bfloat16))
    real, imag, power = (
        lax.dot_general(
            jnp.concatenate(side, axis=1),
            table[...],
            (((1,), (1,)), ((), ())),
            preferred_element_type=jnp.float32,
        )
        for side, table in zip(sides, (re_ref, im_ref, pw_ref))
    )
    total_ref[...] += power - 2.0 * (real + imag)


def match_first(arrived_ref, weight_ref, re_ref, im_ref, pw_ref, total_ref):
    @pl.when(pl.program_id(0) == 0)
    def _():
        total_ref[...] = jnp.zeros_like(total_ref)

    accumulate(arrived_ref, weight_ref, re_ref, im_ref, pw_ref, total_ref)


def match_last(
    arrived_ref, weight_ref, re_ref, im_ref, pw_ref, base_ref, near_ref, out_ref, total_ref
):
    @pl.when(pl.program_id(0) == 0)
    def _():
        total_ref[...] = base_ref[...]

    accumulate(arrived_ref, weight_ref, re_ref, im_ref, pw_ref, total_ref)

    @pl.when(pl.program_id(0) == pl.num_programs(0) - 1)
    def _():
        rows = total_ref.shape[0]
        high, low = (
            near_ref[:, at].reshape(rows, NEAR).astype(jnp.float32).astype(jnp.int32)
            for at in range(2)
        )
        near = 2 * high + low
        lane, band = near & (LANES - 1), near >> 7
        picked = jnp.zeros(near.shape, jnp.float32)
        for at in range(total_ref.shape[1] // LANES):
            piece = total_ref[:, at * LANES : (at + 1) * LANES]
            found = jnp.take_along_axis(piece, lane, axis=1)
            picked = jnp.where(band == at, found, picked)
        picked = picked * (1.0 / math.sqrt(PIX))
        picked = picked - jnp.mean(picked, axis=1, keepdims=True)
        out_ref[...] = picked.reshape(out_ref.shape)


def match(chunk, arrived, weight, tables, base=None):
    devices, depth, slots, _ = arrived.shape
    width = SLABS // CHUNKS
    steps = width // GROUP
    orients = tables[0].shape[0]
    rows = devices * slots
    table = pl.BlockSpec((orients, GROUP * LANES), lambda i: (0, chunk * steps + i))
    full = pl.BlockSpec((rows, orients), lambda i: (0, 0))
    in_specs = [
        pl.BlockSpec((devices, 3 * GROUP, slots, LANES), lambda i: (0, i, 0, 0)),
        pl.BlockSpec((1, GROUP * LANES), lambda i: (0, chunk * steps + i)),
        table,
        table,
        table,
    ]
    common = dict(
        grid=(steps,),
        cost_estimate=pl.CostEstimate(
            flops=2 * rows * orients * depth * LANES,
            bytes_accessed=2 * depth * LANES * (rows + orients),
            transcendentals=0,
        ),
        compiler_params=pltpu.CompilerParams(vmem_limit_bytes=48 * 2**20),
        name=f"match_{chunk}",
    )
    if base is None:
        return pl.pallas_call(
            match_first,
            in_specs=in_specs,
            out_specs=full,
            out_shape=jax.ShapeDtypeStruct((rows, orients), jnp.float32),
            **common,
        )(arrived, weight, *tables)
    extra = pl.BlockSpec((devices, 2, slots, LANES), lambda i: (0, 3 * width // 2, 0, 0))
    return pl.pallas_call(
        match_last,
        in_specs=in_specs + [full, extra],
        out_specs=pl.BlockSpec((devices, slots, NEAR), lambda i: (0, 0, 0)),
        out_shape=jax.ShapeDtypeStruct((devices, slots, NEAR), jnp.float32),
        scratch_shapes=[pltpu.VMEM((rows, orients), jnp.float32)],
        **common,
    )(arrived, weight, *tables, base, arrived)


def per_device(images, ctf, shifts, home, neighbours, references, noise_weight):
    groups = home.shape[0]
    owners = lax.axis_size("orient")
    devices = groups * owners
    local = images.shape[0]
    slots = max(2, 2 * local // owners)
    total = devices * slots
    target = home[:, :, 0]
    earlier = jnp.arange(local)[:, None] > jnp.arange(local)[None, :]
    same = target[:, :, None] == target[:, None, :]
    rank = jnp.sum((same & earlier[None]).astype(jnp.int32), axis=2)
    slot = (jnp.arange(groups, dtype=jnp.int32)[:, None] * owners + target) * slots + rank
    near = neighbours.reshape(local, -1)

    def exchange(array):
        return lax.all_to_all(array, ("grp", "orient"), split_axis=0, concat_axis=0, tiled=True)

    sent = [pack(c, shifts, slot, images, ctf, near, devices, slots) for c in range(CHUNKS)]
    arrived = exchange(sent[0])
    tables = tabulate(references[0], sent[0])
    last, tables = lax.optimization_barrier((sent[1], tables))
    arrived_last = exchange(last)
    score = match(0, arrived, noise_weight, tables)
    scored = match(1, arrived_last, noise_weight, tables, score)
    returned = exchange(scored).reshape(total, -1)
    chosen = (
        slot.T.reshape(-1)[:, None] == jnp.arange(total, dtype=jnp.int32)[None, :]
    ).astype(jnp.float32)
    return jnp.dot(chosen, returned, precision=lax.Precision.HIGHEST).reshape(local, groups, -1)


def solution(mesh):
    in_specs = (
        P(("grp", "orient"), None, None),
        P(("grp", "orient"), None),
        P(("grp", "orient"), None),
        P(None, ("grp", "orient"), None),
        P(("grp", "orient"), None, None),
        P("grp", "orient", None, None),
        P("grp", None),
    )
    out_specs = P(("grp", "orient"), None, None)
    return jax.shard_map(
        per_device, mesh=mesh, in_specs=in_specs, out_specs=out_specs, check_vma=False
    )
```

```python
import math

import jax
import jax.numpy as jnp
from jax import lax
from jax.experimental import pallas as pl
from jax.experimental.pallas import tpu as pltpu
from jax.sharding import PartitionSpec as P

BOX = 128
PIX = 8192
LANES = 128
SLABS = PIX // LANES
CHUNKS = 2
GROUP = 8
NEAR = 128


def rotation(move_x, move_y, slab):
    lane = lax.broadcasted_iota(jnp.int32, move_x.shape, 1)
    row = 2 * slab + jnp.where(lane >= 64, 1, 0) - jnp.where(slab >= SLABS // 2, BOX, 0)
    turns = move_x * (lane & 63).astype(jnp.float32) + move_y * row.astype(jnp.float32)
    quarter = jnp.round(turns * (1.0 / 32.0))
    phi = (turns - 32.0 * quarter) * (2.0 * math.pi / BOX)
    sq = phi * phi
    sine = phi * (1.0 + sq * (-1.0 / 6 + sq * (1.0 / 120 + sq * (-1.0 / 5040 + sq * (1.0 / 362880)))))
    cosine = 1.0 + sq * (-0.5 + sq * (1.0 / 24 + sq * (-1.0 / 720 + sq * (1.0 / 40320))))
    step = quarter.astype(jnp.int32) & 3
    swap = (step & 1) == 1
    base_c = jnp.where(swap, sine, cosine)
    base_s = jnp.where(swap, cosine, sine)
    return (
        jnp.where((step == 1) | (step == 2), -base_c, base_c),
        jnp.where(step >= 2, -base_s, base_s),
    )


def pack_kernel(chunk, width, shift_ref, home_ref, image_ref, ctf_ref, *refs):
    *near_refs, out_ref, held, pair, sems = refs
    local = shift_ref.shape[0]
    groups = home_ref.shape[0]
    devices, depth, slots, _ = out_ref.shape
    share = devices // groups
    step_planes = 3 * GROUP
    move_x = jnp.broadcast_to(shift_ref[:, 0:1].astype(jnp.float32), (local, LANES))
    move_y = jnp.broadcast_to(shift_ref[:, 1:2].astype(jnp.float32), (local, LANES))
    row = lax.broadcasted_iota(jnp.int32, (share * slots, local), 0)
    hit = jnp.concatenate(
        [
            jnp.where(row // slots == home_ref[g : g + 1, :], 1.0, 0.0)
            for g in range(groups)
        ],
        axis=0,
    )
    before = lax.broadcasted_iota(jnp.int32, (local, local), 0)
    after = lax.broadcasted_iota(jnp.int32, (local, local), 1)
    earlier = jnp.where(before < after, 1.0, 0.0).astype(jnp.bfloat16)
    rank = jnp.dot(hit.astype(jnp.bfloat16), earlier, preferred_element_type=jnp.float32)
    row = lax.broadcasted_iota(jnp.int32, hit.shape, 0)
    mine = rank == (row % slots).astype(jnp.float32)
    select = jnp.where(mine, hit, 0.0).astype(jnp.bfloat16)

    def send(i):
        planes = pl.ds(i * step_planes, step_planes)
        return pltpu.make_async_copy(held.at[:, planes], out_ref.at[:, planes], sems.at[i])

    def one(i, carry):
        sides = ([], [], [])
        for r in range(GROUP):
            at = i * GROUP + r
            cols = pl.ds(pl.multiple_of(at * LANES, LANES), LANES)
            cosine, sine = rotation(move_x, move_y, chunk * width + at)
            pair[r] = image_ref[:, :, cols].reshape(2 * local, LANES).astype(jnp.float32)
            real = pair[r, pl.ds(0, local, stride=2), :]
            imag = pair[r, pl.ds(1, local, stride=2), :]
            sides[0].append((real * cosine + imag * sine).astype(jnp.bfloat16))
            sides[1].append((imag * cosine - real * sine).astype(jnp.bfloat16))
            sides[2].append(ctf_ref[:, cols])
        for r in range(0, GROUP, 2):
            payload = jnp.concatenate([side[r + k] for k in range(2) for side in sides], axis=1)
            packed = jnp.dot(select, payload, preferred_element_type=jnp.float32).astype(
                jnp.bfloat16
            )
            for k in range(2):
                for part in range(3):
                    column = (3 * k + part) * LANES
                    held[:, i * step_planes + part * GROUP + r + k] = packed[
                        :, column : column + LANES
                    ].reshape(devices, slots, LANES)
        send(i).start()
        return carry

    steps = width // GROUP
    lax.fori_loop(0, steps, one, 0)
    if near_refs:
        halves = ([], [])
        for g in range(groups):
            chosen = select[g * share * slots : (g + 1) * share * slots]
            near = near_refs[0][:, g * NEAR : (g + 1) * NEAR]
            for half, value in zip(halves, (near >> 1, near & 1)):
                half.append(
                    jnp.dot(
                        chosen,
                        value.astype(jnp.float32).astype(jnp.bfloat16),
                        preferred_element_type=jnp.float32,
                    ).astype(jnp.bfloat16)
                )
        for at, half in enumerate(halves):
            held[:, 3 * width + at] = jnp.concatenate(half, axis=0).reshape(devices, slots, NEAR)
        tail = pl.ds(3 * width, 2)
        rest = pltpu.make_async_copy(held.at[:, tail], out_ref.at[:, tail], sems.at[steps])
        rest.start()
        rest.wait()
    for i in range(steps):
        send(i).wait()


def pack(chunk, shifts, home, images, ctf, near, devices, slots):
    local = shifts.shape[0]
    width = SLABS // CHUNKS
    span = width * LANES
    extra = 2 if chunk == CHUNKS - 1 else 0
    shape = (devices, 3 * width + extra, slots, LANES)
    more = (near,) if extra else ()
    whole = lambda array: pl.BlockSpec(array.shape, lambda i: (0, 0))

    def body(*refs):
        pack_kernel(chunk, width, *refs)

    return pl.pallas_call(
        body,
        grid=(1,),
        in_specs=[
            whole(shifts),
            whole(home),
            pl.BlockSpec((local, 2, span), lambda i: (0, 0, chunk)),
            pl.BlockSpec((local, span), lambda i: (0, chunk)),
            *(whole(array) for array in more),
        ],
        out_specs=pl.BlockSpec(memory_space=pl.ANY),
        out_shape=jax.ShapeDtypeStruct(shape, jnp.bfloat16),
        scratch_shapes=[
            pltpu.VMEM(shape, jnp.bfloat16),
            pltpu.VMEM((GROUP, 2 * local, LANES), jnp.float32),
            pltpu.SemaphoreType.DMA((width // GROUP + 1,)),
        ],
        cost_estimate=pl.CostEstimate(
            flops=2 * devices * slots * local * shape[1] * LANES,
            bytes_accessed=2 * shape[1] * LANES * (devices * slots + local),
            transcendentals=0,
        ),
        compiler_params=pltpu.CompilerParams(vmem_limit_bytes=63 * 2**20),
        name=f"pack_{chunk}",
    )(shifts, home, images, ctf, *more)


def table_kernel(block_ref, after_ref, re_ref, im_ref, pw_ref, pair_ref):
    rows, _, span = block_ref.shape

    def one(r, carry):
        cols = pl.ds(pl.multiple_of(r * LANES, LANES), LANES)
        pair_ref[...] = block_ref[:, :, cols].reshape(2 * rows, LANES).astype(jnp.float32)
        real = pair_ref[pl.ds(0, rows, stride=2), :]
        imag = pair_ref[pl.ds(1, rows, stride=2), :]
        re_ref[:, cols] = real.astype(jnp.bfloat16)
        im_ref[:, cols] = imag.astype(jnp.bfloat16)
        pw_ref[:, cols] = (real * real + imag * imag).astype(jnp.bfloat16)
        return carry

    lax.fori_loop(0, span // LANES, one, 0, unroll=4)


def tabulate(blocks, after):
    orients = blocks.shape[0]
    rows = 64
    out = pl.BlockSpec((rows, PIX), lambda i: (i, 0))
    return pl.pallas_call(
        table_kernel,
        grid=(orients // rows,),
        in_specs=[
            pl.BlockSpec((rows, 2, PIX), lambda i: (i, 0, 0)),
            pl.BlockSpec(memory_space=pl.ANY),
        ],
        out_specs=[out] * 3,
        out_shape=[jax.ShapeDtypeStruct((orients, PIX), jnp.bfloat16)] * 3,
        scratch_shapes=[pltpu.VMEM((2 * rows, LANES), jnp.float32)],
        cost_estimate=pl.CostEstimate(
            flops=2 * orients * PIX * 1024, bytes_accessed=10 * orients * PIX, transcendentals=0
        ),
        name="tabulate",
    )(blocks, after)


def accumulate(arrived_ref, weight_ref, re_ref, im_ref, pw_ref, total_ref):
    rows = total_ref.shape[0]
    sides = ([], [], [])
    for r in range(GROUP):
        real, imag, ctf = (
            arrived_ref[:, part * GROUP + r].reshape(rows, LANES).astype(jnp.float32)
            for part in range(3)
        )
        tone = ctf * weight_ref[:, r * LANES : (r + 1) * LANES]
        for side, value in zip(sides, (real, imag, ctf)):
            side.append((tone * value).astype(jnp.bfloat16))
    real, imag, power = (
        lax.dot_general(
            jnp.concatenate(side, axis=1),
            table[...],
            (((1,), (1,)), ((), ())),
            preferred_element_type=jnp.float32,
        )
        for side, table in zip(sides, (re_ref, im_ref, pw_ref))
    )
    total_ref[...] += power - 2.0 * (real + imag)


def match_first(arrived_ref, weight_ref, re_ref, im_ref, pw_ref, total_ref):
    @pl.when(pl.program_id(0) == 0)
    def _():
        total_ref[...] = jnp.zeros_like(total_ref)

    accumulate(arrived_ref, weight_ref, re_ref, im_ref, pw_ref, total_ref)


def match_last(
    arrived_ref, weight_ref, re_ref, im_ref, pw_ref, base_ref, near_ref, out_ref, total_ref
):
    @pl.when(pl.program_id(0) == 0)
    def _():
        total_ref[...] = base_ref[...]

    accumulate(arrived_ref, weight_ref, re_ref, im_ref, pw_ref, total_ref)

    @pl.when(pl.program_id(0) == pl.num_programs(0) - 1)
    def _():
        rows = total_ref.shape[0]
        high, low = (
            near_ref[:, at].reshape(rows, NEAR).astype(jnp.float32).astype(jnp.int32)
            for at in range(2)
        )
        near = 2 * high + low
        lane, band = near & (LANES - 1), near >> 7
        picked = jnp.zeros(near.shape, jnp.float32)
        for at in range(total_ref.shape[1] // LANES):
            piece = total_ref[:, at * LANES : (at + 1) * LANES]
            found = jnp.take_along_axis(piece, lane, axis=1)
            picked = jnp.where(band == at, found, picked)
        picked = picked * (1.0 / math.sqrt(PIX))
        picked = picked - jnp.mean(picked, axis=1, keepdims=True)
        out_ref[...] = picked.reshape(out_ref.shape)


def match(chunk, arrived, weight, tables, base=None):
    devices, depth, slots, _ = arrived.shape
    width = SLABS // CHUNKS
    steps = width // GROUP
    orients = tables[0].shape[0]
    rows = devices * slots
    table = pl.BlockSpec((orients, GROUP * LANES), lambda i: (0, chunk * steps + i))
    full = pl.BlockSpec((rows, orients), lambda i: (0, 0))
    in_specs = [
        pl.BlockSpec((devices, 3 * GROUP, slots, LANES), lambda i: (0, i, 0, 0)),
        pl.BlockSpec((1, GROUP * LANES), lambda i: (0, chunk * steps + i)),
        table,
        table,
        table,
    ]
    common = dict(
        grid=(steps,),
        cost_estimate=pl.CostEstimate(
            flops=2 * rows * orients * depth * LANES,
            bytes_accessed=2 * depth * LANES * (rows + orients),
            transcendentals=0,
        ),
        compiler_params=pltpu.CompilerParams(vmem_limit_bytes=48 * 2**20),
        name=f"match_{chunk}",
    )
    if base is None:
        return pl.pallas_call(
            match_first,
            in_specs=in_specs,
            out_specs=full,
            out_shape=jax.ShapeDtypeStruct((rows, orients), jnp.float32),
            **common,
        )(arrived, weight, *tables)
    extra = pl.BlockSpec((devices, 2, slots, LANES), lambda i: (0, 3 * width // 2, 0, 0))
    return pl.pallas_call(
        match_last,
        in_specs=in_specs + [full, extra],
        out_specs=pl.BlockSpec((devices, slots, NEAR), lambda i: (0, 0, 0)),
        out_shape=jax.ShapeDtypeStruct((devices, slots, NEAR), jnp.float32),
        scratch_shapes=[pltpu.VMEM((rows, orients), jnp.float32)],
        **common,
    )(arrived, weight, *tables, base, arrived)


def per_device(images, ctf, shifts, home, neighbours, references, noise_weight):
    groups = home.shape[0]
    owners = lax.axis_size("orient")
    devices = groups * owners
    local = images.shape[0]
    slots = max(2, 2 * local // owners)
    total = devices * slots
    target = home[:, :, 0]
    earlier = jnp.arange(local)[:, None] > jnp.arange(local)[None, :]
    same = target[:, :, None] == target[:, None, :]
    rank = jnp.sum((same & earlier[None]).astype(jnp.int32), axis=2)
    slot = (jnp.arange(groups, dtype=jnp.int32)[:, None] * owners + target) * slots + rank
    near = neighbours.reshape(local, -1)

    def exchange(array):
        return lax.all_to_all(array, ("grp", "orient"), split_axis=0, concat_axis=0, tiled=True)

    sent = [pack(c, shifts, target, images, ctf, near, devices, slots) for c in range(CHUNKS)]
    arrived = exchange(sent[0])
    tables = tabulate(references[0], sent[0])
    last, tables = lax.optimization_barrier((sent[1], tables))
    arrived_last = exchange(last)
    score = match(0, arrived, noise_weight, tables)
    scored = match(1, arrived_last, noise_weight, tables, score)
    returned = exchange(scored).reshape(total, -1)
    chosen = (
        slot.T.reshape(-1)[:, None] == jnp.arange(total, dtype=jnp.int32)[None, :]
    ).astype(jnp.float32)
    return jnp.dot(chosen, returned, precision=lax.Precision.HIGHEST).reshape(local, groups, -1)


def solution(mesh):
    in_specs = (
        P(("grp", "orient"), None, None),
        P(("grp", "orient"), None),
        P(("grp", "orient"), None),
        P(None, ("grp", "orient"), None),
        P(("grp", "orient"), None, None),
        P("grp", "orient", None, None),
        P("grp", None),
    )
    out_specs = P(("grp", "orient"), None, None)
    return jax.shard_map(
        per_device, mesh=mesh, in_specs=in_specs, out_specs=out_specs, check_vma=False
    )
```

```python
import math

import jax
import jax.numpy as jnp
from jax import lax
from jax.experimental import pallas as pl
from jax.experimental.pallas import tpu as pltpu
from jax.sharding import PartitionSpec as P

BOX = 128
PIX = 8192
LANES = 128
SLABS = PIX // LANES
WIDTHS = (48, 16)
GROUP = 8
NEAR = 128


def rotation(move_x, move_y, slab):
    lane = lax.broadcasted_iota(jnp.int32, move_x.shape, 1)
    row = 2 * slab + jnp.where(lane >= 64, 1, 0) - jnp.where(slab >= SLABS // 2, BOX, 0)
    turns = move_x * (lane & 63).astype(jnp.float32) + move_y * row.astype(jnp.float32)
    quarter = jnp.round(turns * (1.0 / 32.0))
    phi = (turns - 32.0 * quarter) * (2.0 * math.pi / BOX)
    sq = phi * phi
    sine = phi * (1.0 + sq * (-1.0 / 6 + sq * (1.0 / 120 + sq * (-1.0 / 5040 + sq * (1.0 / 362880)))))
    cosine = 1.0 + sq * (-0.5 + sq * (1.0 / 24 + sq * (-1.0 / 720 + sq * (1.0 / 40320))))
    step = quarter.astype(jnp.int32) & 3
    swap = (step & 1) == 1
    base_c = jnp.where(swap, sine, cosine)
    base_s = jnp.where(swap, cosine, sine)
    return (
        jnp.where((step == 1) | (step == 2), -base_c, base_c),
        jnp.where(step >= 2, -base_s, base_s),
    )


def pack_kernel(first, width, shift_ref, home_ref, image_ref, ctf_ref, *refs):
    *near_refs, out_ref, held, pair, sems = refs
    local = shift_ref.shape[1]
    groups = home_ref.shape[0]
    devices, depth, slots, _ = out_ref.shape
    share = devices // groups
    step_planes = 3 * GROUP
    before = lax.broadcasted_iota(jnp.int32, (local, local), 0)
    after = lax.broadcasted_iota(jnp.int32, (local, local), 1)
    move_x, move_y = (
        jnp.broadcast_to(
            jnp.sum(
                jnp.where(before == after, shift_ref[axis : axis + 1, :].astype(jnp.float32), 0.0),
                axis=1,
                keepdims=True,
            ),
            (local, LANES),
        )
        for axis in range(2)
    )
    row = lax.broadcasted_iota(jnp.int32, (share * slots, local), 0)
    hit = jnp.concatenate(
        [
            jnp.where(row // slots == home_ref[g : g + 1, :], 1.0, 0.0)
            for g in range(groups)
        ],
        axis=0,
    )
    earlier = jnp.where(before < after, 1.0, 0.0).astype(jnp.bfloat16)
    rank = jnp.dot(hit.astype(jnp.bfloat16), earlier, preferred_element_type=jnp.float32)
    row = lax.broadcasted_iota(jnp.int32, hit.shape, 0)
    mine = rank == (row % slots).astype(jnp.float32)
    select = jnp.where(mine, hit, 0.0).astype(jnp.bfloat16)

    def send(i):
        planes = pl.ds(i * step_planes, step_planes)
        return pltpu.make_async_copy(held.at[:, planes], out_ref.at[:, planes], sems.at[i])

    def one(i, carry):
        sides = ([], [], [])
        for r in range(GROUP):
            at = i * GROUP + r
            cols = pl.ds(pl.multiple_of(at * LANES, LANES), LANES)
            cosine, sine = rotation(move_x, move_y, first + at)
            pair[r] = image_ref[:, :, cols].reshape(2 * local, LANES).astype(jnp.float32)
            real = pair[r, pl.ds(0, local, stride=2), :]
            imag = pair[r, pl.ds(1, local, stride=2), :]
            sides[0].append((real * cosine + imag * sine).astype(jnp.bfloat16))
            sides[1].append((imag * cosine - real * sine).astype(jnp.bfloat16))
            sides[2].append(ctf_ref[:, cols])
        for r in range(0, GROUP, 2):
            payload = jnp.concatenate([side[r + k] for k in range(2) for side in sides], axis=1)
            packed = jnp.dot(select, payload, preferred_element_type=jnp.float32).astype(
                jnp.bfloat16
            )
            for k in range(2):
                for part in range(3):
                    column = (3 * k + part) * LANES
                    held[:, i * step_planes + part * GROUP + r + k] = packed[
                        :, column : column + LANES
                    ].reshape(devices, slots, LANES)
        send(i).start()
        return carry

    steps = width // GROUP
    lax.fori_loop(0, steps, one, 0)
    if near_refs:
        halves = ([], [])
        for g in range(groups):
            chosen = select[g * share * slots : (g + 1) * share * slots]
            near = near_refs[0][:, g * NEAR : (g + 1) * NEAR]
            for half, value in zip(halves, (near >> 1, near & 1)):
                half.append(
                    jnp.dot(
                        chosen,
                        value.astype(jnp.float32).astype(jnp.bfloat16),
                        preferred_element_type=jnp.float32,
                    ).astype(jnp.bfloat16)
                )
        for at, half in enumerate(halves):
            held[:, 3 * width + at] = jnp.concatenate(half, axis=0).reshape(devices, slots, NEAR)
        tail = pl.ds(3 * width, 2)
        rest = pltpu.make_async_copy(held.at[:, tail], out_ref.at[:, tail], sems.at[steps])
        rest.start()
        rest.wait()
    for i in range(steps):
        send(i).wait()


def pack(chunk, shifts, home, images, ctf, near, devices, slots):
    local = shifts.shape[0]
    shifts = shifts.T
    width = WIDTHS[chunk]
    at = sum(WIDTHS[:chunk]) // width
    span = width * LANES
    extra = 2 if chunk == len(WIDTHS) - 1 else 0
    shape = (devices, 3 * width + extra, slots, LANES)
    more = (near,) if extra else ()
    whole = lambda array: pl.BlockSpec(array.shape, lambda i: (0, 0))

    def body(*refs):
        pack_kernel(sum(WIDTHS[:chunk]), width, *refs)

    return pl.pallas_call(
        body,
        grid=(1,),
        in_specs=[
            whole(shifts),
            whole(home),
            pl.BlockSpec((local, 2, span), lambda i: (0, 0, at)),
            pl.BlockSpec((local, span), lambda i: (0, at)),
            *(whole(array) for array in more),
        ],
        out_specs=pl.BlockSpec(memory_space=pl.ANY),
        out_shape=jax.ShapeDtypeStruct(shape, jnp.bfloat16),
        scratch_shapes=[
            pltpu.VMEM(shape, jnp.bfloat16),
            pltpu.VMEM((GROUP, 2 * local, LANES), jnp.float32),
            pltpu.SemaphoreType.DMA((width // GROUP + 1,)),
        ],
        cost_estimate=pl.CostEstimate(
            flops=2 * devices * slots * local * shape[1] * LANES,
            bytes_accessed=2 * shape[1] * LANES * (devices * slots + local),
            transcendentals=0,
        ),
        compiler_params=pltpu.CompilerParams(vmem_limit_bytes=63 * 2**20),
        name=f"pack_{chunk}",
    )(shifts, home, images, ctf, *more)


def table_kernel(block_ref, after_ref, re_ref, im_ref, pw_ref, pair_ref):
    rows, _, span = block_ref.shape

    def one(r, carry):
        cols = pl.ds(pl.multiple_of(r * LANES, LANES), LANES)
        pair_ref[...] = block_ref[:, :, cols].reshape(2 * rows, LANES).astype(jnp.float32)
        real = pair_ref[pl.ds(0, rows, stride=2), :]
        imag = pair_ref[pl.ds(1, rows, stride=2), :]
        re_ref[:, cols] = real.astype(jnp.bfloat16)
        im_ref[:, cols] = imag.astype(jnp.bfloat16)
        pw_ref[:, cols] = (real * real + imag * imag).astype(jnp.bfloat16)
        return carry

    lax.fori_loop(0, span // LANES, one, 0, unroll=4)


def tabulate(blocks, after):
    orients = blocks.shape[0]
    rows = 64
    out = pl.BlockSpec((rows, PIX), lambda i: (i, 0))
    return pl.pallas_call(
        table_kernel,
        grid=(orients // rows,),
        in_specs=[
            pl.BlockSpec((rows, 2, PIX), lambda i: (i, 0, 0)),
            pl.BlockSpec(memory_space=pl.ANY),
        ],
        out_specs=[out] * 3,
        out_shape=[jax.ShapeDtypeStruct((orients, PIX), jnp.bfloat16)] * 3,
        scratch_shapes=[pltpu.VMEM((2 * rows, LANES), jnp.float32)],
        cost_estimate=pl.CostEstimate(
            flops=2 * orients * PIX * 1024, bytes_accessed=10 * orients * PIX, transcendentals=0
        ),
        name="tabulate",
    )(blocks, after)


def accumulate(arrived_ref, weight_ref, re_ref, im_ref, pw_ref, total_ref):
    rows = total_ref.shape[0]
    sides = ([], [], [])
    for r in range(GROUP):
        real, imag, ctf = (
            arrived_ref[:, part * GROUP + r].reshape(rows, LANES).astype(jnp.float32)
            for part in range(3)
        )
        tone = ctf * weight_ref[:, r * LANES : (r + 1) * LANES]
        for side, value in zip(sides, (real, imag, ctf)):
            side.append((tone * value).astype(jnp.bfloat16))
    real, imag, power = (
        lax.dot_general(
            jnp.concatenate(side, axis=1),
            table[...],
            (((1,), (1,)), ((), ())),
            preferred_element_type=jnp.float32,
        )
        for side, table in zip(sides, (re_ref, im_ref, pw_ref))
    )
    total_ref[...] += power - 2.0 * (real + imag)


def match_first(arrived_ref, weight_ref, re_ref, im_ref, pw_ref, total_ref):
    @pl.when(pl.program_id(0) == 0)
    def _():
        total_ref[...] = jnp.zeros_like(total_ref)

    accumulate(arrived_ref, weight_ref, re_ref, im_ref, pw_ref, total_ref)


def match_last(
    arrived_ref, weight_ref, re_ref, im_ref, pw_ref, base_ref, near_ref, out_ref, total_ref
):
    @pl.when(pl.program_id(0) == 0)
    def _():
        total_ref[...] = base_ref[...]

    accumulate(arrived_ref, weight_ref, re_ref, im_ref, pw_ref, total_ref)

    @pl.when(pl.program_id(0) == pl.num_programs(0) - 1)
    def _():
        rows = total_ref.shape[0]
        high, low = (
            near_ref[:, at].reshape(rows, NEAR).astype(jnp.float32).astype(jnp.int32)
            for at in range(2)
        )
        near = 2 * high + low
        lane, band = near & (LANES - 1), near >> 7
        picked = jnp.zeros(near.shape, jnp.float32)
        for at in range(total_ref.shape[1] // LANES):
            piece = total_ref[:, at * LANES : (at + 1) * LANES]
            found = jnp.take_along_axis(piece, lane, axis=1)
            picked = jnp.where(band == at, found, picked)
        picked = picked * (1.0 / math.sqrt(PIX))
        picked = picked - jnp.mean(picked, axis=1, keepdims=True)
        out_ref[...] = picked.reshape(out_ref.shape)


def match(chunk, arrived, weight, tables, base=None):
    devices, depth, slots, _ = arrived.shape
    width = WIDTHS[chunk]
    steps = width // GROUP
    done = sum(WIDTHS[:chunk]) // GROUP
    orients = tables[0].shape[0]
    rows = devices * slots
    table = pl.BlockSpec((orients, GROUP * LANES), lambda i: (0, done + i))
    full = pl.BlockSpec((rows, orients), lambda i: (0, 0))
    in_specs = [
        pl.BlockSpec((devices, 3 * GROUP, slots, LANES), lambda i: (0, i, 0, 0)),
        pl.BlockSpec((1, GROUP * LANES), lambda i: (0, done + i)),
        table,
        table,
        table,
    ]
    common = dict(
        grid=(steps,),
        cost_estimate=pl.CostEstimate(
            flops=2 * rows * orients * depth * LANES,
            bytes_accessed=2 * depth * LANES * (rows + orients),
            transcendentals=0,
        ),
        compiler_params=pltpu.CompilerParams(vmem_limit_bytes=63 * 2**20),
        name=f"match_{chunk}",
    )
    if base is None:
        return pl.pallas_call(
            match_first,
            in_specs=in_specs,
            out_specs=full,
            out_shape=jax.ShapeDtypeStruct((rows, orients), jnp.float32),
            **common,
        )(arrived, weight, *tables)
    extra = pl.BlockSpec((devices, 2, slots, LANES), lambda i: (0, 3 * width // 2, 0, 0))
    return pl.pallas_call(
        match_last,
        in_specs=in_specs + [full, extra],
        out_specs=pl.BlockSpec((devices, slots, NEAR), lambda i: (0, 0, 0)),
        out_shape=jax.ShapeDtypeStruct((devices, slots, NEAR), jnp.float32),
        scratch_shapes=[pltpu.VMEM((rows, orients), jnp.float32)],
        **common,
    )(arrived, weight, *tables, base, arrived)


def per_device(images, ctf, shifts, home, neighbours, references, noise_weight):
    groups = home.shape[0]
    owners = lax.axis_size("orient")
    devices = groups * owners
    local = images.shape[0]
    slots = max(2, 2 * local // owners)
    total = devices * slots
    target = home[:, :, 0]
    earlier = jnp.arange(local)[:, None] > jnp.arange(local)[None, :]
    same = target[:, :, None] == target[:, None, :]
    rank = jnp.sum((same & earlier[None]).astype(jnp.int32), axis=2)
    slot = (jnp.arange(groups, dtype=jnp.int32)[:, None] * owners + target) * slots + rank
    near = neighbours.reshape(local, -1)

    def exchange(array):
        return lax.all_to_all(array, ("grp", "orient"), split_axis=0, concat_axis=0, tiled=True)

    sent = [pack(c, shifts, target, images, ctf, near, devices, slots) for c in range(len(WIDTHS))]
    arrived = exchange(sent[0])
    tables = tabulate(references[0], sent[0])
    last, tables = lax.optimization_barrier((sent[1], tables))
    arrived_last = exchange(last)
    score = match(0, arrived, noise_weight, tables)
    scored = match(1, arrived_last, noise_weight, tables, score)
    returned = exchange(scored).reshape(total, -1)
    chosen = (
        slot.T.reshape(-1)[:, None] == jnp.arange(total, dtype=jnp.int32)[None, :]
    ).astype(jnp.float32)
    return jnp.dot(chosen, returned, precision=lax.Precision.HIGHEST).reshape(local, groups, -1)


def solution(mesh):
    in_specs = (
        P(("grp", "orient"), None, None),
        P(("grp", "orient"), None),
        P(("grp", "orient"), None),
        P(None, ("grp", "orient"), None),
        P(("grp", "orient"), None, None),
        P("grp", "orient", None, None),
        P("grp", None),
    )
    out_specs = P(("grp", "orient"), None, None)
    return jax.shard_map(
        per_device, mesh=mesh, in_specs=in_specs, out_specs=out_specs, check_vma=False
    )
```

```python
import math

import jax
import jax.numpy as jnp
from jax import lax
from jax.experimental import pallas as pl
from jax.experimental.pallas import tpu as pltpu
from jax.sharding import PartitionSpec as P

BOX = 128
PIX = 8192
LANES = 128
SLABS = PIX // LANES
WIDTHS = (32, 32)
GROUP = 8
NEAR = 128


def rotation(move_x, move_y, slab):
    lane = lax.broadcasted_iota(jnp.int32, move_x.shape, 1)
    row = 2 * slab + jnp.where(lane >= 64, 1, 0) - jnp.where(slab >= SLABS // 2, BOX, 0)
    turns = move_x * (lane & 63).astype(jnp.float32) + move_y * row.astype(jnp.float32)
    quarter = jnp.round(turns * (1.0 / 32.0))
    phi = (turns - 32.0 * quarter) * (2.0 * math.pi / BOX)
    sq = phi * phi
    sine = phi * (1.0 + sq * (-1.0 / 6 + sq * (1.0 / 120 + sq * (-1.0 / 5040 + sq * (1.0 / 362880)))))
    cosine = 1.0 + sq * (-0.5 + sq * (1.0 / 24 + sq * (-1.0 / 720 + sq * (1.0 / 40320))))
    step = quarter.astype(jnp.int32) & 3
    swap = (step & 1) == 1
    base_c = jnp.where(swap, sine, cosine)
    base_s = jnp.where(swap, cosine, sine)
    return (
        jnp.where((step == 1) | (step == 2), -base_c, base_c),
        jnp.where(step >= 2, -base_s, base_s),
    )


def pack_kernel(first, width, shift_ref, home_ref, image_ref, ctf_ref, *refs):
    *near_refs, out_ref, held, pair, sems = refs
    local = shift_ref.shape[1]
    groups = home_ref.shape[0]
    devices, depth, slots, _ = out_ref.shape
    share = devices // groups
    step_planes = 3 * GROUP
    before = lax.broadcasted_iota(jnp.int32, (local, local), 0)
    after = lax.broadcasted_iota(jnp.int32, (local, local), 1)
    move_x, move_y = (
        jnp.broadcast_to(
            jnp.sum(
                jnp.where(before == after, shift_ref[axis : axis + 1, :].astype(jnp.float32), 0.0),
                axis=1,
                keepdims=True,
            ),
            (local, LANES),
        )
        for axis in range(2)
    )
    row = lax.broadcasted_iota(jnp.int32, (share * slots, local), 0)
    hit = jnp.concatenate(
        [
            jnp.where(row // slots == home_ref[g : g + 1, :], 1.0, 0.0)
            for g in range(groups)
        ],
        axis=0,
    )
    earlier = jnp.where(before < after, 1.0, 0.0).astype(jnp.bfloat16)
    rank = jnp.dot(hit.astype(jnp.bfloat16), earlier, preferred_element_type=jnp.float32)
    row = lax.broadcasted_iota(jnp.int32, hit.shape, 0)
    mine = rank == (row % slots).astype(jnp.float32)
    select = jnp.where(mine, hit, 0.0).astype(jnp.bfloat16)

    def send(i):
        planes = pl.ds(i * step_planes, step_planes)
        return pltpu.make_async_copy(held.at[:, planes], out_ref.at[:, planes], sems.at[i])

    def one(i, carry):
        sides = ([], [], [])
        for r in range(GROUP):
            at = i * GROUP + r
            cols = pl.ds(pl.multiple_of(at * LANES, LANES), LANES)
            cosine, sine = rotation(move_x, move_y, first + at)
            pair[r] = image_ref[:, :, cols].reshape(2 * local, LANES).astype(jnp.float32)
            real = pair[r, pl.ds(0, local, stride=2), :]
            imag = pair[r, pl.ds(1, local, stride=2), :]
            sides[0].append((real * cosine + imag * sine).astype(jnp.bfloat16))
            sides[1].append((imag * cosine - real * sine).astype(jnp.bfloat16))
            sides[2].append(ctf_ref[:, cols])
        for r in range(0, GROUP, 2):
            payload = jnp.concatenate([side[r + k] for k in range(2) for side in sides], axis=1)
            packed = jnp.dot(select, payload, preferred_element_type=jnp.float32).astype(
                jnp.bfloat16
            )
            for k in range(2):
                for part in range(3):
                    column = (3 * k + part) * LANES
                    held[:, i * step_planes + part * GROUP + r + k] = packed[
                        :, column : column + LANES
                    ].reshape(devices, slots, LANES)
        send(i).start()
        return carry

    steps = width // GROUP
    lax.fori_loop(0, steps, one, 0)
    if near_refs:
        halves = ([], [])
        for g in range(groups):
            chosen = select[g * share * slots : (g + 1) * share * slots]
            near = near_refs[0][:, g * NEAR : (g + 1) * NEAR]
            for half, value in zip(halves, (near >> 1, near & 1)):
                half.append(
                    jnp.dot(
                        chosen,
                        value.astype(jnp.float32).astype(jnp.bfloat16),
                        preferred_element_type=jnp.float32,
                    ).astype(jnp.bfloat16)
                )
        for at, half in enumerate(halves):
            held[:, 3 * width + at] = jnp.concatenate(half, axis=0).reshape(devices, slots, NEAR)
        tail = pl.ds(3 * width, 2)
        rest = pltpu.make_async_copy(held.at[:, tail], out_ref.at[:, tail], sems.at[steps])
        rest.start()
        rest.wait()
    for i in range(steps):
        send(i).wait()


def pack(chunk, shifts, home, images, ctf, near, devices, slots):
    local = shifts.shape[0]
    shifts = shifts.T
    width = WIDTHS[chunk]
    at = sum(WIDTHS[:chunk]) // width
    span = width * LANES
    extra = 2 if chunk == len(WIDTHS) - 1 else 0
    shape = (devices, 3 * width + extra, slots, LANES)
    more = (near,) if extra else ()
    whole = lambda array: pl.BlockSpec(array.shape, lambda i: (0, 0))

    def body(*refs):
        pack_kernel(sum(WIDTHS[:chunk]), width, *refs)

    return pl.pallas_call(
        body,
        grid=(1,),
        in_specs=[
            whole(shifts),
            whole(home),
            pl.BlockSpec((local, 2, span), lambda i: (0, 0, at)),
            pl.BlockSpec((local, span), lambda i: (0, at)),
            *(whole(array) for array in more),
        ],
        out_specs=pl.BlockSpec(memory_space=pl.ANY),
        out_shape=jax.ShapeDtypeStruct(shape, jnp.bfloat16),
        scratch_shapes=[
            pltpu.VMEM(shape, jnp.bfloat16),
            pltpu.VMEM((GROUP, 2 * local, LANES), jnp.float32),
            pltpu.SemaphoreType.DMA((width // GROUP + 1,)),
        ],
        cost_estimate=pl.CostEstimate(
            flops=2 * devices * slots * local * shape[1] * LANES,
            bytes_accessed=2 * shape[1] * LANES * (devices * slots + local),
            transcendentals=0,
        ),
        compiler_params=pltpu.CompilerParams(vmem_limit_bytes=63 * 2**20),
        name=f"pack_{chunk}",
    )(shifts, home, images, ctf, *more)


def table_kernel(block_ref, after_ref, re_ref, im_ref, pw_ref, pair_ref):
    rows, _, span = block_ref.shape

    def one(r, carry):
        cols = pl.ds(pl.multiple_of(r * LANES, LANES), LANES)
        pair_ref[...] = block_ref[:, :, cols].reshape(2 * rows, LANES).astype(jnp.float32)
        real = pair_ref[pl.ds(0, rows, stride=2), :]
        imag = pair_ref[pl.ds(1, rows, stride=2), :]
        re_ref[:, cols] = real.astype(jnp.bfloat16)
        im_ref[:, cols] = imag.astype(jnp.bfloat16)
        pw_ref[:, cols] = (real * real + imag * imag).astype(jnp.bfloat16)
        return carry

    lax.fori_loop(0, span // LANES, one, 0, unroll=4)


def tabulate(blocks, after):
    orients = blocks.shape[0]
    rows = 64
    out = pl.BlockSpec((rows, PIX), lambda i: (i, 0))
    return pl.pallas_call(
        table_kernel,
        grid=(orients // rows,),
        in_specs=[
            pl.BlockSpec((rows, 2, PIX), lambda i: (i, 0, 0)),
            pl.BlockSpec(memory_space=pl.ANY),
        ],
        out_specs=[out] * 3,
        out_shape=[jax.ShapeDtypeStruct((orients, PIX), jnp.bfloat16)] * 3,
        scratch_shapes=[pltpu.VMEM((2 * rows, LANES), jnp.float32)],
        cost_estimate=pl.CostEstimate(
            flops=2 * orients * PIX * 1024, bytes_accessed=10 * orients * PIX, transcendentals=0
        ),
        name="tabulate",
    )(blocks, after)


def accumulate(arrived_ref, weight_ref, re_ref, im_ref, pw_ref, total_ref):
    rows = total_ref.shape[0]
    sides = ([], [], [])
    for r in range(GROUP):
        real, imag, ctf = (
            arrived_ref[:, part * GROUP + r].reshape(rows, LANES).astype(jnp.float32)
            for part in range(3)
        )
        tone = ctf * weight_ref[:, r * LANES : (r + 1) * LANES]
        for side, value in zip(sides, (real, imag, ctf)):
            side.append((tone * value).astype(jnp.bfloat16))
    real, imag, power = (
        lax.dot_general(
            jnp.concatenate(side, axis=1),
            table[...],
            (((1,), (1,)), ((), ())),
            preferred_element_type=jnp.float32,
        )
        for side, table in zip(sides, (re_ref, im_ref, pw_ref))
    )
    total_ref[...] += power - 2.0 * (real + imag)


def match_first(arrived_ref, weight_ref, re_ref, im_ref, pw_ref, total_ref):
    @pl.when(pl.program_id(0) == 0)
    def _():
        total_ref[...] = jnp.zeros_like(total_ref)

    accumulate(arrived_ref, weight_ref, re_ref, im_ref, pw_ref, total_ref)


def match_last(
    arrived_ref, weight_ref, re_ref, im_ref, pw_ref, base_ref, near_ref, out_ref, total_ref
):
    @pl.when(pl.program_id(0) == 0)
    def _():
        total_ref[...] = base_ref[...]

    accumulate(arrived_ref, weight_ref, re_ref, im_ref, pw_ref, total_ref)

    @pl.when(pl.program_id(0) == pl.num_programs(0) - 1)
    def _():
        rows = total_ref.shape[0]
        high, low = (
            near_ref[:, at].reshape(rows, NEAR).astype(jnp.float32).astype(jnp.int32)
            for at in range(2)
        )
        near = 2 * high + low
        lane, band = near & (LANES - 1), near >> 7
        picked = jnp.zeros(near.shape, jnp.float32)
        for at in range(total_ref.shape[1] // LANES):
            piece = total_ref[:, at * LANES : (at + 1) * LANES]
            found = jnp.take_along_axis(piece, lane, axis=1)
            picked = jnp.where(band == at, found, picked)
        picked = picked * (1.0 / math.sqrt(PIX))
        picked = picked - jnp.mean(picked, axis=1, keepdims=True)
        out_ref[...] = picked.reshape(out_ref.shape)


def match(chunk, arrived, weight, tables, base=None):
    devices, depth, slots, _ = arrived.shape
    width = WIDTHS[chunk]
    steps = width // GROUP
    done = sum(WIDTHS[:chunk]) // GROUP
    orients = tables[0].shape[0]
    rows = devices * slots
    table = pl.BlockSpec((orients, GROUP * LANES), lambda i: (0, done + i))
    full = pl.BlockSpec((rows, orients), lambda i: (0, 0))
    in_specs = [
        pl.BlockSpec((devices, 3 * GROUP, slots, LANES), lambda i: (0, i, 0, 0)),
        pl.BlockSpec((1, GROUP * LANES), lambda i: (0, done + i)),
        table,
        table,
        table,
    ]
    common = dict(
        grid=(steps,),
        cost_estimate=pl.CostEstimate(
            flops=2 * rows * orients * depth * LANES,
            bytes_accessed=2 * depth * LANES * (rows + orients),
            transcendentals=0,
        ),
        compiler_params=pltpu.CompilerParams(vmem_limit_bytes=48 * 2**20),
        name=f"match_{chunk}",
    )
    if base is None:
        return pl.pallas_call(
            match_first,
            in_specs=in_specs,
            out_specs=full,
            out_shape=jax.ShapeDtypeStruct((rows, orients), jnp.float32),
            **common,
        )(arrived, weight, *tables)
    extra = pl.BlockSpec((devices, 2, slots, LANES), lambda i: (0, 3 * width // 2, 0, 0))
    return pl.pallas_call(
        match_last,
        in_specs=in_specs + [full, extra],
        out_specs=pl.BlockSpec((devices, slots, NEAR), lambda i: (0, 0, 0)),
        out_shape=jax.ShapeDtypeStruct((devices, slots, NEAR), jnp.float32),
        scratch_shapes=[pltpu.VMEM((rows, orients), jnp.float32)],
        **common,
    )(arrived, weight, *tables, base, arrived)


def per_device(images, ctf, shifts, home, neighbours, references, noise_weight):
    groups = home.shape[0]
    owners = lax.axis_size("orient")
    devices = groups * owners
    local = images.shape[0]
    slots = max(2, 2 * local // owners)
    total = devices * slots
    target = home[:, :, 0]
    earlier = jnp.arange(local)[:, None] > jnp.arange(local)[None, :]
    same = target[:, :, None] == target[:, None, :]
    rank = jnp.sum((same & earlier[None]).astype(jnp.int32), axis=2)
    slot = (jnp.arange(groups, dtype=jnp.int32)[:, None] * owners + target) * slots + rank
    near = neighbours.reshape(local, -1)

    def exchange(array):
        return lax.all_to_all(array, ("grp", "orient"), split_axis=0, concat_axis=0, tiled=True)

    sent = [pack(c, shifts, target, images, ctf, near, devices, slots) for c in range(len(WIDTHS))]
    arrived = exchange(sent[0])
    tables = tabulate(references[0], sent[0])
    last, tables = lax.optimization_barrier((sent[1], tables))
    arrived_last = exchange(last)
    score = match(0, arrived, noise_weight, tables)
    scored = match(1, arrived_last, noise_weight, tables, score)
    returned = exchange(scored).reshape(total, -1)
    chosen = (
        slot.T.reshape(-1)[:, None] == jnp.arange(total, dtype=jnp.int32)[None, :]
    ).astype(jnp.float32)
    return jnp.dot(chosen, returned, precision=lax.Precision.HIGHEST).reshape(local, groups, -1)


def solution(mesh):
    in_specs = (
        P(("grp", "orient"), None, None),
        P(("grp", "orient"), None),
        P(("grp", "orient"), None),
        P(None, ("grp", "orient"), None),
        P(("grp", "orient"), None, None),
        P("grp", "orient", None, None),
        P("grp", None),
    )
    out_specs = P(("grp", "orient"), None, None)
    return jax.shard_map(
        per_device, mesh=mesh, in_specs=in_specs, out_specs=out_specs, check_vma=False
    )
```
